32 devices in a mesh: row: 8 (over y, x, core), col: 4 (over z).
Axes of the slice: x: 2, y: 2, z: 4, core: 2. Of those that a mesh axis runs over, the one named last changes fastest.
Arguments:
- rho_real: float32 [8192, 8192], P('row', 'col'), may hold values from -6 to 12, as said below
- rho_imag: float32 [8192, 8192], P('row', 'col'), may hold values from -6 to 6, as said below
- gate_real_matrix: float32 [16, 16], replicated, may hold values from -1 to 1, as said below
- gate_imaginary: float32 [16, 16], replicated, may hold values from -1 to 1, as said below
- angles: float32 [8, 3], replicated, may hold values from -3.140625 to 3.140625
- targets: int32 [8], replicated, may hold values from 0 to 4
- gate_order: int32 [8], replicated, may hold values from 0 to 7, each once
Outputs:
- mixed_real: float32 [8192, 8192], P('row', 'col')
- depolarized_quadrature: float32 [8192, 8192], P('row', 'col')
- purity: float32 [], replicated
The draws below stay inside these ranges and needn't reach their ends.
Inputs may be any that keep to these rules, and one draw needn't show every extreme that they name: rho_real is symmetric: entries of order one off the diagonal, each diagonal entry raised by 2 to 6. rho_imag is antisymmetric with a zero diagonal, so that rho_real + i rho_imag is Hermitian. gate_real_matrix + i gate_imaginary is a unitary matrix. gate_real_matrix + i gate_imaginary is a unitary matrix. `targets`: each gate acts on one of the 5 low qubits. `gate_order`: each gate appears once.
All inputs are finite; a program needn't handle non-finite values.
Results may differ from the reference program's by a relative error of at most 0.0001.
Values sent between devices are 32-bit elements; how exact they have to be, the bound alone decides.
A program may use at most 128 MiB of HBM per device.

```python
import jax
import jax.numpy as jnp
from jax import lax

LQ = 5
GATE = 16
GATES = 8
DIM = 8192


def mirrored_weights(key):
    return jnp.ones((DIM,), jnp.float32)


def raw_noise(key):
    return jnp.clip(jax.random.normal(key, (DIM, DIM), jnp.float32), -6.0, 6.0)


def draw_rho_real(key, part):
    noise_key = jax.random.fold_in(key, 11)
    scale_key = jax.random.fold_in(key, 12)
    raise_key = jax.random.fold_in(key, 13)
    values = raw_noise(noise_key)
    values = 0.5 * (values + values.T)
    scales = mirrored_weights(scale_key)
    values = values * scales[:, None] * scales[None, :]
    raises = jax.random.uniform(raise_key, (DIM,), jnp.float32, 2.0, 6.0)
    on_diag = lax.broadcasted_iota(jnp.int32, (DIM, DIM), 0) == lax.broadcasted_iota(jnp.int32, (DIM, DIM), 1)
    return values + jnp.where(on_diag, raises[None, :], jnp.zeros_like(values))


def draw_rho_imag(key, part):
    noise_key = jax.random.fold_in(key, 21)
    scale_key = jax.random.fold_in(key, 22)
    values = raw_noise(noise_key)
    values = 0.5 * (values - values.T)
    scales = mirrored_weights(scale_key)
    return values * scales[:, None] * scales[None, :]


def unitary_parts(key):
    shared = jax.random.fold_in(key, 31)
    real_key = jax.random.fold_in(shared, 1)
    imag_key = jax.random.fold_in(shared, 2)
    first = jax.random.normal(real_key, (GATE, GATE), jnp.float32)
    second = jax.random.normal(imag_key, (GATE, GATE), jnp.float32)
    whole = lax.complex(first, second)
    factor_q, factor_r = jnp.linalg.qr(whole)
    diag_r = jnp.diagonal(factor_r)
    phases = diag_r / jnp.maximum(jnp.abs(diag_r), 0.001)
    unitary = factor_q * phases[None, :]
    return (jnp.real(unitary).astype(jnp.float32), jnp.imag(unitary).astype(jnp.float32))


def draw_gate_real_matrix(key, part):
    return unitary_parts(key)[0]


def draw_gate_imaginary(key, part):
    return unitary_parts(key)[1]


def place_ends(array, stream_key, low, largest):
    shape = array.shape
    spot = [jax.random.randint(jax.random.fold_in(stream_key, axis), (), 0, shape[axis]) for axis in range(len(shape))]
    array = array.at[tuple(spot)].set(low)
    longest = shape.index(max(shape))
    spot[longest] = (spot[longest] + 1) % shape[longest]
    return array.at[tuple(spot)].set(largest)


def setup_inputs(seed: int = 0) -> dict:
    splits = jax.random.split(jax.random.key(seed), 8)
    rho_real = draw_rho_real(jax.random.fold_in(splits[7], 71), 0)
    rho_imag = draw_rho_imag(jax.random.fold_in(splits[7], 71), 0)
    gate_real_matrix = draw_gate_real_matrix(jax.random.fold_in(splits[7], 71), 0)
    gate_imaginary = draw_gate_imaginary(jax.random.fold_in(splits[7], 71), 0)
    angles = jnp.clip(jax.random.uniform(splits[4], (GATES, 3), jnp.float32, -3.140625, 3.140625), -3.140625, 3.140625)
    targets = place_ends(jax.random.randint(splits[5], (GATES,), 0, LQ), jax.random.fold_in(splits[5], 1), 0, LQ - 1).astype(jnp.int32)
    gate_order = jax.random.permutation(splits[6], GATES).astype(jnp.int32)
    return dict(rho_real=rho_real, rho_imag=rho_imag, gate_real_matrix=gate_real_matrix, gate_imaginary=gate_imaginary, angles=angles, targets=targets, gate_order=gate_order)


highest = lax.Precision.HIGHEST
mixing = 0.25

def complex_blend(pattern, left_real, left_imag, right_real, right_imag):
    real_part = jnp.einsum(pattern, left_real, right_real, precision=highest) - jnp.einsum(pattern, left_imag, right_imag, precision=highest)
    imag_part = jnp.einsum(pattern, left_real, right_imag, precision=highest) + jnp.einsum(pattern, left_imag, right_real, precision=highest)
    return (real_part, imag_part)

def embed_gate(angle_row, target, low_width):
    half_turn = angle_row[0] / 2
    cosine_half = jnp.cos(half_turn)
    sine_half = jnp.sin(half_turn)
    phase_first = angle_row[1]
    phase_second = angle_row[2]
    element_count = ((cosine_half, cosine_half * 0.0), (-jnp.cos(phase_second) * sine_half, -jnp.sin(phase_second) * sine_half), (jnp.cos(phase_first) * sine_half, jnp.sin(phase_first) * sine_half), (jnp.cos(phase_first + phase_second) * cosine_half, jnp.sin(phase_first + phase_second) * cosine_half))
    left_index = lax.broadcasted_iota(jnp.int32, (low_width, low_width), 0)
    right_index = lax.broadcasted_iota(jnp.int32, (low_width, low_width), 1)
    target_bit = jnp.left_shift(jnp.ones((), jnp.int32), target.astype(jnp.int32))
    same_rest = jnp.bitwise_or(jnp.bitwise_xor(left_index, right_index), target_bit) == target_bit
    left_high = jnp.bitwise_and(left_index, target_bit) > 0
    right_high = jnp.bitwise_and(right_index, target_bit) > 0
    result = []
    for member in range(2):
        chosen = jnp.where(left_high, jnp.where(right_high, element_count[3][member], element_count[2][member]), jnp.where(right_high, element_count[1][member], element_count[0][member]))
        result.append(jnp.where(same_rest, chosen, jnp.zeros_like(chosen)))
    return (result[0], result[1])

def joined_gate(angles, targets, gate_order, low_width):
    gate_count = angles.shape[0]
    slot_ids = jnp.arange(gate_count, dtype=jnp.int32)
    total_real = jnp.eye(low_width, dtype=jnp.float32)
    total_imag = jnp.zeros((low_width, low_width), jnp.float32)
    for position in range(gate_count):
        picked = slot_ids == gate_order[position].astype(jnp.int32)
        angle_row = jnp.sum(jnp.where(picked[:, None], angles, jnp.zeros_like(angles)), axis=0)
        target = jnp.sum(jnp.where(picked, targets, jnp.zeros_like(targets))).astype(jnp.int32)
        step_real, step_imag = embed_gate(angle_row, target, low_width)
        total_real, total_imag = complex_blend('ab,bc->ac', step_real, step_imag, total_real, total_imag)
    return (total_real, total_imag)

def reference(rho_real, rho_imag, gate_real_matrix, gate_imaginary, angles, targets, gate_order):
    low_width = 2 ** LQ
    block_inphase_component, block_quadrature = joined_gate(angles, targets, gate_order, low_width)

    def row_block(segment_list):
        center_divide = complex_blend('xi,ifo->xfo', gate_real_matrix, gate_imaginary, segment_list[0], segment_list[1])
        return complex_blend('hf,ofg->ohg', block_inphase_component, block_quadrature, center_divide[0], center_divide[1])
    split_real = jnp.transpose(rho_real.reshape(GATE, GATE, low_width, DIM), (1, 0, 2, 3))
    split_imag = jnp.transpose(rho_imag.reshape(GATE, GATE, low_width, DIM), (1, 0, 2, 3))
    rows_real, rows_imag = lax.map(row_block, (split_real, split_imag))

    def col_block(segment_list):
        center_divide = complex_blend('rghl,Gg->rhGl', segment_list[0], segment_list[1], gate_real_matrix, -gate_imaginary)
        return complex_blend('rhGl,Ll->rhGL', center_divide[0], center_divide[1], block_inphase_component, -block_quadrature)
    block_rows = 512
    block_count = DIM // block_rows
    col_real, col_imag = lax.map(col_block, (rows_real.reshape(block_count, block_rows, GATE, GATE, low_width), rows_imag.reshape(block_count, block_rows, GATE, GATE, low_width)))
    col_real = col_real.reshape(DIM, DIM)
    col_imag = col_imag.reshape(DIM, DIM)
    trace_real = jnp.trace(col_real)
    trace_imag = jnp.trace(col_imag)
    diag_index = jnp.arange(DIM, dtype=jnp.int32)
    mixed_real = ((1 - mixing) * col_real).at[diag_index, diag_index].add(mixing * trace_real / DIM)
    depolarized_quadrature = ((1 - mixing) * col_imag).at[diag_index, diag_index].add(mixing * trace_imag / DIM)
    purity = (jnp.sum(mixed_real * mixed_real) + jnp.sum(depolarized_quadrature * depolarized_quadrature)) / (DIM * DIM)
    return (mixed_real, depolarized_quadrature, purity)
```

```python
import functools

import jax
import jax.numpy as jnp
from jax import lax
from jax.experimental import pallas as pl
from jax.experimental.pallas import tpu as pltpu
from jax.sharding import PartitionSpec as P

LQ = 5
GATE = 16
DIM = 8192


highest = lax.Precision.HIGHEST
mixing = 0.25


def complex_blend(pattern, left_real, left_imag, right_real, right_imag):
    real_part = jnp.einsum(pattern, left_real, right_real, precision=highest) - jnp.einsum(
        pattern, left_imag, right_imag, precision=highest
    )
    imag_part = jnp.einsum(pattern, left_real, right_imag, precision=highest) + jnp.einsum(
        pattern, left_imag, right_real, precision=highest
    )
    return (real_part, imag_part)


def embed_gate(angle_row, target, low_width):
    half_turn = angle_row[0] / 2
    cosine_half = jnp.cos(half_turn)
    sine_half = jnp.sin(half_turn)
    phase_first = angle_row[1]
    phase_second = angle_row[2]
    element_count = (
        (cosine_half, cosine_half * 0.0),
        (-jnp.cos(phase_second) * sine_half, -jnp.sin(phase_second) * sine_half),
        (jnp.cos(phase_first) * sine_half, jnp.sin(phase_first) * sine_half),
        (
            jnp.cos(phase_first + phase_second) * cosine_half,
            jnp.sin(phase_first + phase_second) * cosine_half,
        ),
    )
    left_index = lax.broadcasted_iota(jnp.int32, (low_width, low_width), 0)
    right_index = lax.broadcasted_iota(jnp.int32, (low_width, low_width), 1)
    target_bit = jnp.left_shift(jnp.ones((), jnp.int32), target)
    same_rest = jnp.bitwise_or(jnp.bitwise_xor(left_index, right_index), target_bit) == target_bit
    left_high = jnp.bitwise_and(left_index, target_bit) > 0
    right_high = jnp.bitwise_and(right_index, target_bit) > 0
    result = []
    for member in range(2):
        chosen = jnp.where(
            left_high,
            jnp.where(right_high, element_count[3][member], element_count[2][member]),
            jnp.where(right_high, element_count[1][member], element_count[0][member]),
        )
        result.append(jnp.where(same_rest, chosen, jnp.zeros_like(chosen)))
    return (result[0], result[1])


def joined_gate(angles, targets, gate_order, low_width):
    gate_count = angles.shape[0]
    slot_ids = jnp.arange(gate_count, dtype=jnp.int32)
    total_real = jnp.eye(low_width, dtype=jnp.float32)
    total_imag = jnp.zeros((low_width, low_width), jnp.float32)
    for position in range(gate_count):
        picked = slot_ids == gate_order[position]
        angle_row = jnp.sum(jnp.where(picked[:, None], angles, jnp.zeros_like(angles)), axis=0)
        target = jnp.sum(jnp.where(picked, targets, jnp.zeros_like(targets)))
        step_real, step_imag = embed_gate(angle_row, target, low_width)
        total_real, total_imag = complex_blend(
            "ab,bc->ac", step_real, step_imag, total_real, total_imag
        )
    return (total_real, total_imag)


def on_device(rho_real, rho_imag, gate_real_matrix, gate_imaginary, angles, targets, gate_order):
    row_count, col_count = rho_real.shape
    low_width = 2**LQ
    row_parts = GATE // lax.axis_size("row")
    col_parts = GATE // lax.axis_size("col")
    block_inphase_component, block_quadrature = joined_gate(angles, targets, gate_order, low_width)
    moved = (
        lax.all_to_all(
            rho_real.reshape(row_parts, GATE, low_width * col_count),
            "row",
            split_axis=1,
            concat_axis=0,
            tiled=True,
        ),
        lax.all_to_all(
            rho_imag.reshape(row_parts, GATE, low_width * col_count),
            "row",
            split_axis=1,
            concat_axis=0,
            tiled=True,
        ),
    )
    center_divide = complex_blend(
        "sx,xazw->aszw",
        gate_real_matrix,
        gate_imaginary,
        moved[0].reshape(GATE, row_parts, low_width, col_count),
        moved[1].reshape(GATE, row_parts, low_width, col_count),
    )
    rotated_state = complex_blend(
        "us,ebsl->ebul",
        block_inphase_component,
        block_quadrature,
        center_divide[0],
        center_divide[1],
    )
    moved = (
        lax.all_to_all(
            rotated_state[0].reshape(row_count, col_parts, GATE * low_width),
            "col",
            split_axis=2,
            concat_axis=1,
            tiled=True,
        ),
        lax.all_to_all(
            rotated_state[1].reshape(row_count, col_parts, GATE * low_width),
            "col",
            split_axis=2,
            concat_axis=1,
            tiled=True,
        ),
    )
    center_divide = complex_blend(
        "rghl,Gg->rhGl",
        moved[0].reshape(row_count, GATE, col_parts, low_width),
        moved[1].reshape(row_count, GATE, col_parts, low_width),
        gate_real_matrix,
        -gate_imaginary,
    )
    final = complex_blend(
        "rhGl,Ll->rhGL",
        center_divide[0],
        center_divide[1],
        block_inphase_component,
        -block_quadrature,
    )
    new_real = final[0].reshape(row_count, col_count)
    updated_quadrature = final[1].reshape(row_count, col_count)
    row_global = lax.axis_index("row") * row_count + lax.broadcasted_iota(
        jnp.int32, (row_count, col_count), 0
    )
    col_global = lax.axis_index("col") * col_count + lax.broadcasted_iota(
        jnp.int32, (row_count, col_count), 1
    )
    diagonal = row_global == col_global
    part_trace_real = jnp.sum(jnp.where(diagonal, new_real, jnp.zeros_like(new_real)))
    part_trace_imag = jnp.sum(
        jnp.where(diagonal, updated_quadrature, jnp.zeros_like(updated_quadrature))
    )
    keep_share = 1 - mixing
    part_squares = jnp.sum(new_real * new_real) + jnp.sum(updated_quadrature * updated_quadrature)
    trace_real, trace_imag, squares = lax.psum(
        (part_trace_real, part_trace_imag, part_squares), ("row", "col")
    )
    shift_real = mixing * trace_real / DIM
    shift_imag = mixing * trace_imag / DIM
    mixed_real = keep_share * new_real + jnp.where(diagonal, shift_real, jnp.zeros_like(new_real))
    depolarized_quadrature = keep_share * updated_quadrature + jnp.where(
        diagonal, shift_imag, jnp.zeros_like(updated_quadrature)
    )
    trace_squared = trace_real * trace_real + trace_imag * trace_imag
    purity = (
        keep_share * keep_share * squares
        + (2 * keep_share * mixing + mixing * mixing) * trace_squared / DIM
    ) / (DIM * DIM)
    return (mixed_real, depolarized_quadrature, purity)


def gather_blocks(shape, real, imag, out, send_sem, recv_sem):
    row_size, col_size, row_parts, col_parts, low_width = shape
    devices = row_size * col_size
    row = lax.axis_index("row")
    col = lax.axis_index("col")
    high = row_parts * low_width
    wide = col_parts * low_width
    stride = GATE * low_width

    def partner(step):
        place = lax.rem(row * col_size + col + step, devices)
        return place // col_size, lax.rem(place, col_size)

    def chunks(to_row, to_col):
        for row_step in range(row_parts):
            for col_step in range(col_parts):
                for member, source in enumerate((real, imag)):
                    yield (
                        source.at[
                            pl.ds(pl.multiple_of(row_step * stride + to_row * high, 8), high),
                            pl.ds(pl.multiple_of(col_step * stride + to_col * wide, 128), wide),
                        ],
                        out.at[
                            member * GATE + row * row_parts + row_step,
                            :,
                            pl.ds(
                                pl.multiple_of((col * col_parts + col_step) * wide, 128), wide
                            ),
                        ],
                    )

    def start_step(step, carry):
        to_row, to_col = partner(step)
        for source, target in chunks(to_row, to_col):
            pltpu.make_async_remote_copy(
                src_ref=source,
                dst_ref=target,
                send_sem=send_sem,
                recv_sem=recv_sem,
                device_id=(to_row, to_col),
                device_id_type=pl.DeviceIdType.MESH,
            ).start()
        return carry

    lax.fori_loop(1, devices, start_step, 0)
    for source, target in chunks(row, col):
        pltpu.make_async_copy(source, target, recv_sem).start()
    sent = out.at[pl.ds(0, 2 * GATE - 2 * GATE // devices)]
    pltpu.make_async_copy(sent, sent, send_sem).wait()
    pltpu.make_async_copy(out, out, recv_sem).wait()


def split_weights(values):
    high = lax.reduce_precision(values, 8, 7)
    low = lax.reduce_precision(values - high, 8, 7)
    return high.astype(jnp.bfloat16), low.astype(jnp.bfloat16)


def split(values):
    high = values.astype(jnp.bfloat16)
    return high, (values - high.astype(jnp.float32)).astype(jnp.bfloat16)


def dot(left, right):
    def one(a, b):
        return jnp.dot(a, b, preferred_element_type=jnp.float32)

    return one(left[0], right[0]) + (one(left[0], right[1]) + one(left[1], right[0]))


def rotate_blocks(shift_ref, held, left_high, left_low, right_high, right_low, real, imag):
    size = real.shape[0]
    row_step = pl.program_id(0)
    col_step = pl.program_id(1)
    low_width = size // GATE
    wide = held.shape[-1] // GATE

    def spread(lane):
        pieces = []
        for member in range(2):
            state = held[member, :, 0].reshape(size, held.shape[-1])
            for part in range(GATE):
                start = part * wide + lane * low_width
                pieces.append(state[:, start : start + low_width])
        return jnp.concatenate(pieces, axis=1)

    def finish(lane):
        state = spread(lane)
        middle = dot(split(state), (right_high[...], right_low[...]))
        stacked = jnp.concatenate([middle[:, :size], middle[:, size:]], axis=0)
        final = dot((left_high[...], left_low[...]), split(stacked))
        rows = shift_ref[2].astype(jnp.int32)
        cols = shift_ref[3].astype(jnp.int32)
        on_diagonal = (
            rows + row_step * size + lax.broadcasted_iota(jnp.int32, (size, size), 0)
        ) == (cols + col_step * size + lax.broadcasted_iota(jnp.int32, (size, size), 1))
        keep_share = 1 - mixing
        zero = jnp.zeros((size, size), jnp.float32)
        real[...] = keep_share * final[:size] + jnp.where(on_diagonal, shift_ref[0], zero)
        imag[...] = keep_share * final[size:] + jnp.where(on_diagonal, shift_ref[1], zero)

    for lane in range(wide // low_width):
        pl.when(col_step == lane)(functools.partial(finish, lane))


def direct(rho_real, rho_imag, gate_real_matrix, gate_imaginary, angles, targets, gate_order):
    row_count, col_count = rho_real.shape
    low_width = 2**LQ
    row_size = lax.axis_size("row")
    col_size = lax.axis_size("col")
    row_parts = GATE // row_size
    col_parts = GATE // col_size
    size = GATE * low_width
    high = row_parts * low_width
    wide = col_parts * low_width
    row_start = lax.axis_index("row") * row_count
    col_start = lax.axis_index("col") * col_count
    diagonal = (row_start + lax.broadcasted_iota(jnp.int32, (row_count, col_count), 0)) == (
        col_start + lax.broadcasted_iota(jnp.int32, (row_count, col_count), 1)
    )
    zero = jnp.zeros_like(rho_real)
    trace_real, trace_imag, squares = lax.psum(
        (
            jnp.sum(jnp.where(diagonal, rho_real, zero)),
            jnp.sum(jnp.where(diagonal, rho_imag, zero)),
            jnp.sum(rho_real * rho_real + rho_imag * rho_imag),
        ),
        ("row", "col"),
    )
    held = pl.pallas_call(
        functools.partial(
            gather_blocks, (row_size, col_size, row_parts, col_parts, low_width)
        ),
        out_shape=jax.ShapeDtypeStruct((2 * GATE, high, GATE * wide), jnp.float32),
        in_specs=[pl.BlockSpec(memory_space=pl.ANY)] * 2,
        out_specs=pl.BlockSpec(memory_space=pl.ANY),
        scratch_shapes=[
            pltpu.SemaphoreType.DMA,
            pltpu.SemaphoreType.DMA,
        ],
        compiler_params=pltpu.CompilerParams(has_side_effects=True),
    )(rho_real, rho_imag)
    local_real, local_imag = joined_gate(angles, targets, gate_order, low_width)

    def kron(first, second):
        return (first[:, None, :, None] * second[None, :, None, :]).reshape(size, size)

    whole_real = kron(gate_real_matrix, local_real) - kron(gate_imaginary, local_imag)
    whole_imag = kron(gate_real_matrix, local_imag) + kron(gate_imaginary, local_real)
    left = jnp.block([[whole_real, -whole_imag], [whole_imag, whole_real]])
    right = jnp.block([[whole_real.T, -whole_imag.T], [whole_imag.T, whole_real.T]])
    shift = jnp.stack(
        [
            mixing * trace_real / DIM,
            mixing * trace_imag / DIM,
            row_start.astype(jnp.float32),
            col_start.astype(jnp.float32),
        ]
    )
    full = pl.BlockSpec((2 * size, 2 * size), lambda i, j: (0, 0))
    block = pl.BlockSpec((size, size), lambda i, j: (i, j))
    mixed_real, depolarized_quadrature = pl.pallas_call(
        rotate_blocks,
        grid=(row_parts, col_parts),
        out_shape=[jax.ShapeDtypeStruct((row_count, col_count), jnp.float32)] * 2,
        in_specs=[
            pl.BlockSpec(memory_space=pltpu.SMEM),
            pl.BlockSpec(
                (2, GATE, 1, low_width, GATE * wide), lambda i, j: (0, 0, i, 0, 0)
            ),
            full,
            full,
            full,
            full,
        ],
        out_specs=[block, block],
        compiler_params=pltpu.CompilerParams(vmem_limit_bytes=60 * 2**20),
    )(
        shift,
        held.reshape(2, GATE, row_parts, low_width, GATE * wide),
        *split_weights(left),
        *split_weights(right),
    )
    keep_share = 1 - mixing
    trace_squared = trace_real * trace_real + trace_imag * trace_imag
    purity = (
        keep_share * keep_share * squares
        + (2 * keep_share * mixing + mixing * mixing) * trace_squared / DIM
    ) / (DIM * DIM)
    return (mixed_real, depolarized_quadrature, purity)


def solution(mesh):
    in_specs = (P("row", "col"), P("row", "col"), P(), P(), P(), P(), P())
    out_specs = (P("row", "col"), P("row", "col"), P())
    col_parts = GATE // mesh.shape["col"]
    row_parts = GATE // mesh.shape["row"]
    aligned = col_parts * 2**LQ % 128 == 0 and mesh.shape["col"] == 4 and row_parts == 2
    return jax.shard_map(
        direct if aligned else on_device,
        mesh=mesh,
        in_specs=in_specs,
        out_specs=out_specs,
        check_vma=False,
    )
```
